32 devices in a mesh: grp: 2 (over y), band: 4 (over x, core), ga: 4 (over z).
Axes of the slice: x: 2, y: 2, z: 4, core: 2. Of those that a mesh axis runs over, the one named last changes fastest.
Arguments:
- orbitals: bfloat16 [64, 8192], P(('grp', 'band'), 'ga'), parts along dimension 0, may hold values from -0.0625 to 0.0625
- energies: float32 [64], P(('grp', 'band')), parts along dimension 0, may hold values from -1.5 to -0.2
- projectors: bfloat16 [1024, 8192], P('grp', 'ga'), parts along dimension 0, may hold values from -0.125 to 0.125
- miller_index: int32 [3, 8192], P(None, 'ga'), may hold values from -12 to 12
- recip_scale: float32 [6], P('grp'), parts along dimension 0, may hold values from 0.06 to 0.14
- species: int32 [128], replicated, may hold values from 0 to 2
- proj_atom: int32 [512], replicated, may hold values from 0 to 127, as said below
- coupling: float32 [3, 4], replicated, may hold values from 0.5 to 3
Outputs:
- response: bfloat16 [3, 64, 8192], P(None, ('grp', 'band'), 'ga'), parts along dimension 1
- dielectric: float32 [6, 3], P('grp'), parts along dimension 0
- born: float32 [9, 256], P(None, 'grp'), parts along dimension 1
The draws below stay inside these ranges and needn't reach their ends.
There are 2 independent parts, one for each index of `grp`. The reference program is written for one: setup_inputs(seed, part) draws one part's arguments, and reference() takes and returns one part's arrays. A program takes and returns all parts, laid end to end along the dimension named above; an argument that names none is the same for every part. Nothing has to cross between parts.
Inputs may be any that keep to these rules, and one draw needn't show every extreme that they name: `proj_atom`: every atom owns exactly 4 projectors.
All inputs are finite; a program needn't handle non-finite values.
Results may differ from the reference program's by a relative error of at most 0.015.
Values may be sent and summed in bfloat16 or wider, within the bound.
A program may use at most 64 MiB of HBM per device.

```python
import math
import jax
import jax.numpy as jnp
from jax import lax

NATOM = 128
PROJ = 4
NSPEC = 3
ITERS = 2
NP = 512
NB = 32
NG = 8192


def draw_proj_atom(key, part):
    order = jax.random.permutation(jax.random.fold_in(key, 17), NP)
    return (order // PROJ).astype(jnp.int32)


def touch_ends(entries, stream_key, smallest, largest):
    dims = entries.shape
    spot = [jax.random.randint(jax.random.fold_in(stream_key, axis), (), 0, dims[axis]) for axis in range(len(dims))]
    entries = entries.at[tuple(spot)].set(smallest)
    longest = dims.index(max(dims))
    spot[longest] = (spot[longest] + 1) % dims[longest]
    return entries.at[tuple(spot)].set(largest)


def shard_levels(rng, extent, split, smallest, largest):
    def one(axis_at, blocks):
        draws = jax.random.uniform(jax.random.fold_in(jax.random.fold_in(rng, 6), axis_at), (blocks,), jnp.float32, smallest / len(split), largest / len(split))
        return jnp.repeat(jnp.exp(draws), extent[axis_at] // blocks).reshape((-1,) + (1,) * (len(extent) - axis_at - 1))

    gain = one(*split[0])
    for cut in split[1:]:
        gain = gain * one(*cut)
    return gain


def bell_draw(rng, shape, width, limit, pieces=(), held_as=jnp.bfloat16):
    array = width * jax.random.normal(rng, shape, jnp.float32)
    if pieces:
        array = array * shard_levels(rng, shape, pieces, -0.22, 0.18)
    return jnp.clip(array, -limit, limit).astype(held_as)


def setup_inputs(seed: int = 0, part: int = 0) -> dict:
    key_list = jax.random.split(jax.random.key(seed), 9)
    part_splits = jax.random.split(jax.random.fold_in(key_list[8], part), 9)
    return {
        "orbitals": bell_draw(part_splits[0], (NB, NG), NG ** -0.5, 0.0625, ((0, 4), (1, 4))),
        "energies": jnp.clip(-1.5 + 1.3 * jax.random.uniform(part_splits[1], (NB,), jnp.float32) ** shard_levels(part_splits[1], (NB,), ((0, 4),), -0.2, 0.2), -1.5, -0.2),
        "projectors": bell_draw(part_splits[2], (NP, NG), ((NP * NG) ** -0.25), 0.125, ((1, 4),)),
        "miller_index": touch_ends(jax.random.randint(key_list[3], (3, NG), -12, 13), jax.random.fold_in(key_list[3], 1), -12, 12).astype(jnp.int32),
        "recip_scale": jnp.clip(jnp.exp(jax.random.uniform(part_splits[4], (3,), jnp.float32, math.log(0.06), math.log(0.14))), 0.06, 0.14),
        "species": touch_ends(jax.random.randint(key_list[5], (NATOM,), 0, NSPEC), jax.random.fold_in(key_list[5], 1), 0, NSPEC - 1).astype(jnp.int32),
        "proj_atom": draw_proj_atom(jax.random.fold_in(key_list[8], 71), part),
        "coupling": jnp.clip(jnp.exp(jax.random.uniform(key_list[7], (NSPEC, PROJ), jnp.float32, math.log(0.5), math.log(3.0))), 0.5, 3.0),
    }


born_scale = 40.0


def tables(miller_index, recip_scale, species, proj_atom, coupling):
    wavevec = miller_index.astype(jnp.float32) * recip_scale[:, None]
    kinetic = 0.5 * jnp.sum(wavevec * wavevec, axis=0)
    atom_onehot = (proj_atom[:, None] == jnp.arange(NATOM, dtype=jnp.int32)[None, :]).astype(jnp.float32)
    spec_proj = jnp.dot(atom_onehot, species.astype(jnp.float32), precision=lax.Precision.HIGHEST)
    spec_onehot = (spec_proj[:, None] == jnp.arange(NSPEC, dtype=jnp.float32)[None, :]).astype(jnp.float32)
    channel = jnp.arange(NP, dtype=jnp.int32) % PROJ
    chan_onehot = (channel[:, None] == jnp.arange(PROJ, dtype=jnp.int32)[None, :]).astype(jnp.float32)
    strength = jnp.sum(jnp.dot(spec_onehot, coupling, precision=lax.Precision.HIGHEST) * chan_onehot, axis=1)
    return wavevec, kinetic, atom_onehot, strength


def conduct(values, orbitals):
    results = []
    for direc in range(3):
        margin = jnp.dot(orbitals, values[direc].T, preferred_element_type=jnp.float32).astype(jnp.bfloat16)
        removed = jnp.dot(margin.T, orbitals, preferred_element_type=jnp.float32)
        results.append(values[direc].astype(jnp.float32) - removed)
    return jnp.stack(results)


def reference(orbitals, energies, projectors, miller_index, recip_scale, species, proj_atom, coupling):
    wavevec, kinetic, atom_onehot, strength = tables(miller_index, recip_scale, species, proj_atom, coupling)
    precond = 1.0 / (1.0 + kinetic)
    orb_float = orbitals.astype(jnp.float32)
    stacked = jnp.concatenate([orb_float[None], wavevec[:, None, :] * orb_float[None]], 0).astype(jnp.bfloat16)
    proj = jnp.dot(stacked.reshape(4 * NB, NG), projectors.T, preferred_element_type=jnp.float32).reshape(4, NB, NP)
    weighted = (strength * proj).astype(jnp.bfloat16)
    returned = jnp.dot(weighted.reshape(4 * NB, NP), projectors, preferred_element_type=jnp.float32).reshape(4, NB, NG)
    commutator = (wavevec[:, None, :] * (orb_float + returned[0])[None] + returned[1:]).astype(jnp.bfloat16)
    source = -conduct(commutator, orbitals)
    response = jnp.zeros_like(source)
    residual = source
    resp_proj = jnp.zeros((3, NB, NP), jnp.float32)
    diag_shift = kinetic[None, None, :] - energies[None, :, None]
    for step in range(ITERS):
        search = conduct((precond * residual).astype(jnp.bfloat16), orbitals)
        search_low = search.astype(jnp.bfloat16)
        dir_proj = jnp.dot(search_low.reshape(3 * NB, NG), projectors.T, preferred_element_type=jnp.float32).reshape(3, NB, NP)
        dir_weight = (strength * dir_proj).astype(jnp.bfloat16)
        image = diag_shift * search + jnp.dot(dir_weight.reshape(3 * NB, NP), projectors, preferred_element_type=jnp.float32).reshape(3, NB, NG)
        numerator = jnp.sum(residual * search, axis=2)
        curvature = jnp.sum(search * image, axis=2)
        step_size = numerator / curvature
        response = response + step_size[:, :, None] * search
        residual = residual - step_size[:, :, None] * image
        resp_proj = resp_proj + step_size[:, :, None] * dir_proj
    dielectric = jnp.eye(3, dtype=jnp.float32) + (4.0 / NB) * jnp.einsum("anx,bnx->ab", response, source, precision=lax.Precision.HIGHEST)
    pair = jnp.einsum("anp,bnp->abp", resp_proj, proj[1:], precision=lax.Precision.HIGHEST)
    born = born_scale * jnp.dot((pair * strength).reshape(9, NP), atom_onehot, precision=lax.Precision.HIGHEST)
    return response.astype(jnp.bfloat16), dielectric, born
```

```python
import functools

import jax
import jax.numpy as jnp
from jax import lax
from jax.experimental import pallas as pl
from jax.experimental.pallas import tpu as pltpu
from jax.sharding import PartitionSpec as P

ITERS = 2
BORN_SCALE = 40.0
MESH = pl.DeviceIdType.MESH
F32 = jnp.float32
BF16 = jnp.bfloat16
NT = (((1,), (1,)), ((), ()))
NN = (((1,), (0,)), ((), ()))


def mm(a, b, dims, precision=None):
    return lax.dot_general(a, b, dims, preferred_element_type=F32, precision=precision)


class Exchange:
    def __init__(self, buf, send, recv, axis, n, me, pick=()):
        self.copies = []
        self.arrivals = []
        for off in range(1, n):
            peer = lax.rem(me + off, n)
            src = buf.at[(me,) + pick]
            self.copies.append(
                pltpu.make_async_remote_copy(
                    src_ref=src,
                    dst_ref=src,
                    send_sem=send.at[off],
                    recv_sem=recv.at[me],
                    device_id={axis: peer},
                    device_id_type=MESH,
                )
            )
            other = buf.at[(peer,) + pick]
            self.arrivals.append(
                pltpu.make_async_remote_copy(
                    src_ref=other,
                    dst_ref=other,
                    send_sem=send.at[off],
                    recv_sem=recv.at[peer],
                    device_id={axis: peer},
                    device_id_type=MESH,
                )
            )

    def start(self):
        for copy in self.copies:
            copy.start()
        return self

    def wait(self):
        for arrival in self.arrivals:
            arrival.wait_recv()

    def drain(self):
        for copy in self.copies:
            copy.wait_send()


def total(buf, n):
    acc = buf[0].astype(F32)
    for j in range(1, n):
        acc = acc + buf[j].astype(F32)
    return acc


def kernel(
    nga,
    nband,
    pchunks,
    orb_ref,
    energy_ref,
    proj_hbm,
    miller_ref,
    recip_ref,
    species_ref,
    atom_ref,
    coupling_ref,
    resp_ref,
    diel_ref,
    born_ref,
    pv,
    oall,
    ofull,
    okall,
    r1,
    kk,
    kall,
    kfull,
    gram,
    r2,
    dir3,
    sm3,
    dir4,
    sm4,
    fin,
    pairs,
    psem,
    *sems,
):
    bands, width = orb_ref.shape
    nproj = pv.shape[0]
    tb = bands * nband
    rows = 3 * bands
    ga = lax.axis_index("ga")
    bd = lax.axis_index("band")
    pc = nproj // pchunks

    barrier = pltpu.get_barrier_semaphore()
    for off in range(1, nga):
        pl.semaphore_signal(
            barrier, inc=1, device_id={"ga": lax.rem(ga + off, nga)}, device_id_type=MESH
        )
    for off in range(1, nband):
        pl.semaphore_signal(
            barrier, inc=1, device_id={"band": lax.rem(bd + off, nband)}, device_id_type=MESH
        )
    loads = []
    for k in range(pchunks):
        part = pl.ds(k * pc, pc)
        loads.append(pltpu.make_async_copy(proj_hbm.at[part], pv.at[part], psem.at[k]))
        loads[-1].start()

    it = iter(sems)

    def exchange(buf, axis, pick=()):
        n, me = (nga, ga) if axis == "ga" else (nband, bd)
        return Exchange(buf, next(it), next(it), axis, n, me, pick)

    orb = orb_ref[...].astype(F32)
    wave = [miller_ref[d : d + 1, :].astype(F32) * recip_ref[d] for d in range(3)]
    kinetic = 0.5 * (wave[0] * wave[0] + wave[1] * wave[1] + wave[2] * wave[2])
    precond = 1.0 / (1.0 + kinetic)
    stacked = jnp.concatenate(
        [orb] + [wave[d] * orb for d in range(3)] + [precond * orb], axis=0
    ).astype(BF16)

    band_row = lax.broadcasted_iota(jnp.int32, (bands, 1), 0)
    ecol = jnp.zeros((bands, 1), F32)
    for n in range(bands):
        ecol = jnp.where(band_row == n, energy_ref[n], ecol)
    shift = kinetic - ecol
    shift = jnp.concatenate([shift] * 3, axis=0)

    natoms = species_ref.shape[1]
    atoms = lax.broadcasted_iota(jnp.int32, (natoms, nproj), 0)
    onehot = (atoms == atom_ref[...]).astype(BF16)
    species = species_ref[...].astype(F32)
    spec_rows = jnp.concatenate([species] * 8, axis=0).astype(BF16)
    spec = mm(spec_rows, onehot, NN)[0:1]
    nspec, nchan = coupling_ref.shape
    chan = lax.rem(lax.broadcasted_iota(jnp.int32, (1, nproj), 1), nchan)
    strength = jnp.zeros((1, nproj), F32)
    for s in range(nspec):
        for c in range(nchan):
            strength = jnp.where(
                jnp.logical_and(spec == float(s), chan == c), coupling_ref[s, c], strength
            )

    pl.semaphore_wait(barrier, nga + nband - 2)

    oall[bd] = orb_ref[...]
    x0 = exchange(oall, "band").start()

    x1 = []
    for k in range(pchunks):
        loads[k].wait()
        part = pl.ds(k * pc, pc)
        piece = mm(stacked, pv[part, :], NT)
        r1[ga, :, part] = piece[: 4 * bands].astype(BF16)
        kk[ga, :, part] = piece[4 * bands :].astype(BF16)
        x1.append(exchange(r1, "ga", (slice(None), part)).start())
    xk = exchange(kk, "ga").start()

    x0.wait()
    for j in range(nband):
        ofull[j * bands : (j + 1) * bands, :] = oall[j].astype(F32)
    occupied = ofull[...].astype(BF16)
    okall[:tb, :] = occupied
    okall[tb:, :] = (precond * ofull[...]).astype(BF16)
    gram[ga] = mm(occupied, okall[tb:, :], NT)
    xg = exchange(gram, "ga").start()

    for x in x1:
        x.wait()
    proj = total(r1, nga)
    weighted = (strength * proj).astype(BF16)
    returned = mm(weighted, pv[...], NN)
    inner = orb + returned[:bands]
    comm = jnp.concatenate(
        [wave[d] * inner + returned[(1 + d) * bands : (2 + d) * bands] for d in range(3)], axis=0
    ).astype(BF16)
    r2[ga] = mm(comm, okall[...], NT)
    x2 = exchange(r2, "ga").start()

    xk.wait()
    kall[bd] = total(kk, nga).astype(BF16)
    xa = exchange(kall, "band").start()

    xg.wait()
    gram_all = total(gram, nga)
    x2.wait()
    both = total(r2, nga)
    margin = both[:, :tb].astype(BF16)
    margin_next = mm(margin.astype(F32), gram_all, NN, lax.Precision.HIGHEST) - both[:, tb:]
    removed = mm(
        jnp.concatenate([margin.astype(F32), margin_next], axis=0).astype(BF16),
        okall[:tb, :],
        NN,
    )
    source = removed[:rows] - comm.astype(F32)
    search = (precond * source).astype(BF16).astype(F32) - removed[rows:]

    def send_direction(found, buf):
        low = found.astype(BF16)
        out = []
        for k in range(pchunks):
            part = pl.ds(k * pc, pc)
            buf[ga, :, part] = mm(low, pv[part, :], NT).astype(BF16)
            out.append(exchange(buf, "ga", (slice(None), part)).start())
        return out

    def overlaps(found):
        return [
            jnp.sum(
                found * jnp.concatenate([source[b * bands : (b + 1) * bands]] * 3, axis=0),
                axis=1,
                keepdims=True,
            )
            for b in range(3)
        ]

    def step_of(buf, small, col):
        dp = total(buf, nga)
        dw = (strength * dp).astype(BF16)
        curvature = small[:, col + 1 : col + 2] + jnp.sum(
            dw.astype(F32) * dp, axis=1, keepdims=True
        )
        return dp, dw, small[:, col : col + 1] / curvature

    x3 = send_direction(search, dir3)
    shifted = shift * search
    sm3[ga, :, :tb] = mm((precond * shifted).astype(BF16), okall[:tb, :], NT)
    sm3[ga, :, tb : tb + 1] = jnp.sum(source * search, axis=1, keepdims=True)
    sm3[ga, :, tb + 1 : tb + 2] = jnp.sum(shifted * search, axis=1, keepdims=True)
    x3.append(exchange(sm3, "ga").start())

    for b, col in enumerate(overlaps(search)):
        sm4[ga, :, 2 + b : 3 + b] = col
    xa.wait()
    for j in range(nband):
        kfull[j * bands : (j + 1) * bands, :] = kall[j].astype(F32)
    kp = kfull[...].astype(BF16)

    for x in x3:
        x.wait()
    small3 = total(sm3, nga)
    dp1, dw1, alpha1 = step_of(dir3, small3, tb)
    image = shifted + mm(dw1, pv[...], NN)
    residual = source - alpha1 * image
    margin3 = margin_next - alpha1 * (small3[:, :tb] + mm(dw1, kp, NT))
    search2 = (precond * residual).astype(BF16).astype(F32) - mm(
        margin3.astype(BF16), okall[:tb, :], NN
    )
    x4 = send_direction(search2, dir4)
    sm4[ga, :, 0:1] = jnp.sum(residual * search2, axis=1, keepdims=True)
    sm4[ga, :, 1:2] = jnp.sum(shift * search2 * search2, axis=1, keepdims=True)
    for b, col in enumerate(overlaps(search2)):
        sm4[ga, :, 5 + b : 6 + b] = col
    x4.append(exchange(sm4, "ga").start())

    for x in x4:
        x.wait()
    small4 = total(sm4, nga)
    dp2, _, alpha2 = step_of(dir4, small4, 0)
    resp_proj = alpha1 * dp1 + alpha2 * dp2
    pairs[...] = jnp.zeros_like(pairs)
    for a in range(3):
        left = resp_proj[a * bands : (a + 1) * bands]
        for b in range(3):
            right = proj[(1 + b) * bands : (2 + b) * bands]
            pairs[3 * a + b : 3 * a + b + 1, :] = strength * jnp.sum(
                left * right, axis=0, keepdims=True
            )
    born = mm(pairs[...], onehot.astype(F32), NT, lax.Precision.HIGHEST)
    diel = alpha1 * small4[:, 2:5] + alpha2 * small4[:, 5:8]
    fin[bd, 0:16, :] = born
    fin[bd, 16:24, :] = jnp.zeros((8, born.shape[1]), F32)
    for a in range(3):
        fin[bd, 16 + a : 17 + a, 0:3] = jnp.sum(
            diel[a * bands : (a + 1) * bands], axis=0, keepdims=True
        )
    xf = exchange(fin, "band").start()
    response = alpha1 * search + alpha2 * search2
    for a in range(3):
        resp_ref[a] = response[a * bands : (a + 1) * bands].astype(BF16)
    xf.wait()
    final = total(fin, nband)
    born_ref[...] = BORN_SCALE * final[0:9]
    eye = (
        lax.broadcasted_iota(jnp.int32, (3, 3), 0) == lax.broadcasted_iota(jnp.int32, (3, 3), 1)
    ).astype(F32)
    diel_ref[...] = eye + (4.0 / tb) * final[16:19, 0:3]

    for x in [x0, *x1, xk, xg, x2, xa, *x3, *x4, xf]:
        x.drain()


def solution(mesh):
    nga, nband = mesh.shape["ga"], mesh.shape["band"]

    def per_device(
        orbitals, energies, projectors, miller_index, recip_scale, species, proj_atom, coupling
    ):
        bands, width = orbitals.shape
        nproj = projectors.shape[0]
        natoms = species.shape[0]
        tb = bands * nband
        rows = 3 * bands
        pchunks = 4
        smw = -(-(tb + 8) // 128) * 128
        axes = ["band"] + ["ga"] * pchunks + ["ga", "ga", "ga", "band"]
        axes += (["ga"] * pchunks + ["ga"]) * 2 + ["band"]
        sems = []
        for axis in axes:
            sems += [pltpu.SemaphoreType.DMA((mesh.shape[axis],))] * 2
        vmem = pl.BlockSpec(memory_space=pltpu.VMEM)
        smem = pl.BlockSpec(memory_space=pltpu.SMEM)
        return pl.pallas_call(
            functools.partial(kernel, nga, nband, pchunks),
            out_shape=(
                jax.ShapeDtypeStruct((3, bands, width), BF16),
                jax.ShapeDtypeStruct((3, 3), F32),
                jax.ShapeDtypeStruct((9, natoms), F32),
            ),
            in_specs=[
                vmem,
                smem,
                pl.BlockSpec(memory_space=pl.ANY),
                vmem,
                smem,
                vmem,
                vmem,
                smem,
            ],
            out_specs=(vmem, vmem, vmem),
            scratch_shapes=[
                pltpu.VMEM((nproj, width), BF16),
                pltpu.VMEM((nband, bands, width), BF16),
                pltpu.VMEM((tb, width), F32),
                pltpu.VMEM((2 * tb, width), BF16),
                pltpu.VMEM((nga, 4 * bands, nproj), BF16),
                pltpu.VMEM((nga, bands, nproj), BF16),
                pltpu.VMEM((nband, bands, nproj), BF16),
                pltpu.VMEM((tb, nproj), F32),
                pltpu.VMEM((nga, tb, tb), F32),
                pltpu.VMEM((nga, rows, 2 * tb), F32),
                pltpu.VMEM((nga, rows, nproj), BF16),
                pltpu.VMEM((nga, rows, smw), F32),
                pltpu.VMEM((nga, rows, nproj), BF16),
                pltpu.VMEM((nga, rows, 128), F32),
                pltpu.VMEM((nband, 24, natoms), F32),
                pltpu.VMEM((16, nproj), F32),
                pltpu.SemaphoreType.DMA((pchunks,)),
                *sems,
            ],
            compiler_params=pltpu.CompilerParams(
                collective_id=0, has_side_effects=True, vmem_limit_bytes=48 * 1024 * 1024
            ),
        )(
            orbitals,
            energies,
            projectors,
            miller_index,
            recip_scale,
            species.reshape(1, natoms),
            proj_atom.reshape(1, nproj),
            coupling,
        )

    placed = (
        P(("grp", "band"), "ga"),
        P(("grp", "band")),
        P("grp", "ga"),
        P(None, "ga"),
        P("grp"),
        P(),
        P(),
        P(),
    )
    return jax.shard_map(
        per_device,
        mesh=mesh,
        in_specs=placed,
        out_specs=(P(None, ("grp", "band"), "ga"), P("grp", None), P(None, "grp")),
        check_vma=False,
    )
```

```python
import functools

import jax
import jax.numpy as jnp
from jax import lax
from jax.experimental import pallas as pl
from jax.experimental.pallas import tpu as pltpu
from jax.sharding import PartitionSpec as P

ITERS = 2
BORN_SCALE = 40.0
MESH = pl.DeviceIdType.MESH
F32 = jnp.float32
BF16 = jnp.bfloat16
NT = (((1,), (1,)), ((), ()))
NN = (((1,), (0,)), ((), ()))


def mm(a, b, dims, precision=None):
    return lax.dot_general(a, b, dims, preferred_element_type=F32, precision=precision)


class Exchange:
    def __init__(self, buf, send, recv, axis, n, me, pick=()):
        self.copies = []
        self.arrivals = []
        for off in range(1, n):
            peer = lax.rem(me + off, n)
            src = buf.at[(me,) + pick]
            self.copies.append(
                pltpu.make_async_remote_copy(
                    src_ref=src,
                    dst_ref=src,
                    send_sem=send.at[off],
                    recv_sem=recv.at[me],
                    device_id={axis: peer},
                    device_id_type=MESH,
                )
            )
            other = buf.at[(peer,) + pick]
            self.arrivals.append(
                pltpu.make_async_remote_copy(
                    src_ref=other,
                    dst_ref=other,
                    send_sem=send.at[off],
                    recv_sem=recv.at[peer],
                    device_id={axis: peer},
                    device_id_type=MESH,
                )
            )

    def start(self):
        for copy in self.copies:
            copy.start()
        return self

    def wait(self):
        for arrival in self.arrivals:
            arrival.wait_recv()

    def drain(self):
        for copy in self.copies:
            copy.wait_send()


def total(buf, n):
    acc = buf[0].astype(F32)
    for j in range(1, n):
        acc = acc + buf[j].astype(F32)
    return acc


def kernel(
    nga,
    nband,
    pchunks,
    orb_hbm,
    energy_hbm,
    proj_hbm,
    miller_hbm,
    recip_hbm,
    species_hbm,
    atom_hbm,
    coupling_hbm,
    resp_ref,
    diel_ref,
    born_ref,
    orb_ref,
    energy_ref,
    miller_ref,
    recip_ref,
    species_ref,
    atom_ref,
    coupling_ref,
    lsem,
    pv,
    oall,
    ofull,
    okall,
    r1,
    kk,
    kall,
    kfull,
    gram,
    gall,
    gfull,
    dir3,
    sm3,
    dir4,
    sm4,
    fin,
    pairs,
    psem,
    *sems,
):
    bands, width = orb_ref.shape
    nproj = pv.shape[0]
    tb = bands * nband
    rows = 3 * bands
    ga = lax.axis_index("ga")
    bd = lax.axis_index("band")
    pc = nproj // pchunks

    barrier = pltpu.get_barrier_semaphore()
    for off in range(1, nga):
        pl.semaphore_signal(
            barrier, inc=1, device_id={"ga": lax.rem(ga + off, nga)}, device_id_type=MESH
        )
    for off in range(1, nband):
        pl.semaphore_signal(
            barrier, inc=1, device_id={"band": lax.rem(bd + off, nband)}, device_id_type=MESH
        )
    small = []
    for i, (src, dst) in enumerate(
        [
            (orb_hbm, orb_ref),
            (miller_hbm, miller_ref),
            (recip_hbm, recip_ref),
            (energy_hbm, energy_ref),
            (species_hbm, species_ref),
            (atom_hbm, atom_ref),
            (coupling_hbm, coupling_ref),
        ]
    ):
        small.append(pltpu.make_async_copy(src, dst, lsem.at[i]))
        small[-1].start()
    loads = []
    for k in range(pchunks):
        part = pl.ds(k * pc, pc)
        loads.append(pltpu.make_async_copy(proj_hbm.at[part], pv.at[part], psem.at[k]))
        loads[-1].start()

    it = iter(sems)

    def exchange(buf, axis, pick=()):
        n, me = (nga, ga) if axis == "ga" else (nband, bd)
        return Exchange(buf, next(it), next(it), axis, n, me, pick)

    for load in small:
        load.wait()
    orb = orb_ref[...].astype(F32)
    wave = [miller_ref[d : d + 1, :].astype(F32) * recip_ref[d] for d in range(3)]
    kinetic = 0.5 * (wave[0] * wave[0] + wave[1] * wave[1] + wave[2] * wave[2])
    precond = 1.0 / (1.0 + kinetic)
    stacked = jnp.concatenate(
        [orb] + [wave[d] * orb for d in range(3)] + [precond * orb], axis=0
    ).astype(BF16)

    band_row = lax.broadcasted_iota(jnp.int32, (bands, 1), 0)
    ecol = jnp.zeros((bands, 1), F32)
    for n in range(bands):
        ecol = jnp.where(band_row == n, energy_ref[n], ecol)
    ecol = jnp.concatenate([ecol] * 3, axis=0)
    shift = kinetic - ecol

    natoms = species_ref.shape[1]
    atoms = lax.broadcasted_iota(jnp.int32, (natoms, nproj), 0)
    onehot = (atoms == atom_ref[...]).astype(BF16)
    species = species_ref[...].astype(F32)
    spec_rows = jnp.concatenate([species] * 8, axis=0).astype(BF16)
    spec = mm(spec_rows, onehot, NN)[0:1]
    nspec, nchan = coupling_ref.shape
    chan = lax.rem(lax.broadcasted_iota(jnp.int32, (1, nproj), 1), nchan)
    strength = jnp.zeros((1, nproj), F32)
    for s in range(nspec):
        for c in range(nchan):
            strength = jnp.where(
                jnp.logical_and(spec == float(s), chan == c), coupling_ref[s, c], strength
            )

    pl.semaphore_wait(barrier, nga + nband - 2)

    oall[bd] = orb_ref[...]
    x0 = exchange(oall, "band").start()

    x1 = []
    for k in range(pchunks):
        loads[k].wait()
        part = pl.ds(k * pc, pc)
        piece = mm(stacked, pv[part, :], NT)
        r1[ga, :, part] = piece[: 4 * bands].astype(BF16)
        kk[ga, :, part] = piece[4 * bands :].astype(BF16)
        x1.append(exchange(r1, "ga", (slice(None), part)).start())
    xk = exchange(kk, "ga").start()

    x0.wait()
    for j in range(nband):
        ofull[j * bands : (j + 1) * bands, :] = oall[j].astype(F32)
    every = ofull[...]
    okall[:tb, :] = every.astype(BF16)
    okall[tb : 2 * tb, :] = (precond * every).astype(BF16)
    okall[2 * tb : 3 * tb, :] = (precond * precond * every).astype(BF16)
    okall[3 * tb :, :] = (kinetic * every).astype(BF16)
    gram[ga] = mm(orb_ref[...], okall[...], NT)
    xg = exchange(gram, "ga").start()

    for x in x1:
        x.wait()
    proj = total(r1, nga)
    weighted = (strength * proj).astype(BF16)
    returned = mm(weighted, pv[...], NN)
    inner = orb + returned[:bands]
    comm = jnp.concatenate(
        [wave[d] * inner + returned[(1 + d) * bands : (2 + d) * bands] for d in range(3)], axis=0
    ).astype(BF16)
    comm_float = comm.astype(F32)

    def send_direction(found, buf):
        low = found.astype(BF16)
        out = []
        for k in range(pchunks):
            part = pl.ds(k * pc, pc)
            buf[ga, :, part] = mm(low, pv[part, :], NT).astype(BF16)
            out.append(exchange(buf, "ga", (slice(None), part)).start())
        return out

    scaled = precond * comm_float
    x3 = send_direction(scaled, dir3)
    sm3[ga, :, : 3 * tb] = mm(comm, okall[: 3 * tb, :], NT)
    sm3[ga, :, 3 * tb : 3 * tb + 1] = jnp.sum(scaled * comm_float, axis=1, keepdims=True)
    sm3[ga, :, 3 * tb + 1 : 3 * tb + 2] = jnp.sum(scaled * scaled, axis=1, keepdims=True)
    x3.append(exchange(sm3, "ga").start())

    xk.wait()
    xg.wait()
    kall[bd, :, :nproj] = proj[:bands].astype(BF16)
    kall[bd, :, nproj:] = total(kk, nga).astype(BF16)
    gall[bd] = total(gram, nga)
    xa = [exchange(kall, "band").start(), exchange(gall, "band").start()]
    for x in xa:
        x.wait()
    for j in range(nband):
        kfull[j * bands : (j + 1) * bands, :] = kall[j].astype(F32)
        gfull[j * bands : (j + 1) * bands, :] = gall[j]
    pp = kfull[:, :nproj].astype(BF16)
    kp = kfull[:, nproj:].astype(BF16)
    grams = gfull[...]
    g1, gk, gk2, gkin = [grams[:, q * tb : (q + 1) * tb] for q in range(4)]

    def hi(a, b):
        return mm(a, b, NN, lax.Precision.HIGHEST)

    for x in x3:
        x.wait()
    small3 = total(sm3, nga)
    u, v, w = [small3[:, q * tb : (q + 1) * tb] for q in range(3)]
    ckc = small3[:, 3 * tb : 3 * tb + 1]
    ck2c = small3[:, 3 * tb + 1 : 3 * tb + 2]
    margin_low = u.astype(BF16)
    margin = margin_low.astype(F32)
    a1k, a2k = hi(margin, gk), hi(margin, gk2)
    margin_next = a1k - v
    next_low = margin_next.astype(BF16)
    nxt = next_low.astype(F32)
    b1, bk, bkin = hi(nxt, g1), hi(nxt, gk), hi(nxt, gkin)
    numerator = ckc + jnp.sum(
        margin * (a1k - 2.0 * v - b1) + nxt * u, axis=1, keepdims=True
    )
    diag = (ckc - ck2c - ecol * ck2c) + jnp.sum(
        margin * (a1k - a2k - 2.0 * (v - w) - 2.0 * (b1 - bk))
        + nxt * (2.0 * (u - v) + bkin)
        - ecol * (margin * (a2k - 2.0 * w - 2.0 * bk) + nxt * (2.0 * v + b1)),
        axis=1,
        keepdims=True,
    )
    margin_step = (a1k - a2k) - (v - w) - (b1 - bk) - ecol * (a2k - w - bk)
    dp1 = mm(margin_low, kp, NN) - mm(next_low, pp, NN) - total(dir3, nga)
    dw1 = (strength * dp1).astype(BF16)
    alpha1 = numerator / (
        diag + jnp.sum(dw1.astype(F32) * dp1, axis=1, keepdims=True)
    )
    removed = mm(jnp.concatenate([margin, nxt], axis=0).astype(BF16), okall[:tb, :], NN)
    source = removed[:rows] - comm_float
    search = precond * source - removed[rows:]

    def overlaps(found):
        return [
            jnp.sum(
                found * jnp.concatenate([source[b * bands : (b + 1) * bands]] * 3, axis=0),
                axis=1,
                keepdims=True,
            )
            for b in range(3)
        ]

    def step_of(buf, small, col):
        dp = total(buf, nga)
        dw = (strength * dp).astype(BF16)
        curvature = small[:, col + 1 : col + 2] + jnp.sum(
            dw.astype(F32) * dp, axis=1, keepdims=True
        )
        return dp, dw, small[:, col : col + 1] / curvature

    shifted = shift * search
    image = shifted + mm(dw1, pv[...], NN)
    residual = source - alpha1 * image
    margin3 = margin_next - alpha1 * (margin_step + mm(dw1, kp, NT))
    search2 = (precond * residual).astype(BF16).astype(F32) - mm(
        margin3.astype(BF16), okall[:tb, :], NN
    )
    x4 = send_direction(search2, dir4)
    for b, col in enumerate(overlaps(search)):
        sm4[ga, :, 2 + b : 3 + b] = col
    sm4[ga, :, 0:1] = jnp.sum(residual * search2, axis=1, keepdims=True)
    sm4[ga, :, 1:2] = jnp.sum(shift * search2 * search2, axis=1, keepdims=True)
    for b, col in enumerate(overlaps(search2)):
        sm4[ga, :, 5 + b : 6 + b] = col
    x4.append(exchange(sm4, "ga").start())

    for x in x4:
        x.wait()
    small4 = total(sm4, nga)
    dp2, _, alpha2 = step_of(dir4, small4, 0)
    resp_proj = alpha1 * dp1 + alpha2 * dp2
    pairs[...] = jnp.zeros_like(pairs)
    for a in range(3):
        left = resp_proj[a * bands : (a + 1) * bands]
        for b in range(3):
            right = proj[(1 + b) * bands : (2 + b) * bands]
            pairs[3 * a + b : 3 * a + b + 1, :] = strength * jnp.sum(
                left * right, axis=0, keepdims=True
            )
    born = mm(pairs[...], onehot.astype(F32), NT, lax.Precision.HIGHEST)
    diel = alpha1 * small4[:, 2:5] + alpha2 * small4[:, 5:8]
    fin[bd, 0:16, :] = born
    fin[bd, 16:24, :] = jnp.zeros((8, born.shape[1]), F32)
    for a in range(3):
        fin[bd, 16 + a : 17 + a, 0:3] = jnp.sum(
            diel[a * bands : (a + 1) * bands], axis=0, keepdims=True
        )
    xf = exchange(fin, "band").start()
    response = alpha1 * search + alpha2 * search2
    for a in range(3):
        resp_ref[a] = response[a * bands : (a + 1) * bands].astype(BF16)
    xf.wait()
    final = total(fin, nband)
    born_ref[...] = BORN_SCALE * final[0:9]
    eye = (
        lax.broadcasted_iota(jnp.int32, (3, 3), 0) == lax.broadcasted_iota(jnp.int32, (3, 3), 1)
    ).astype(F32)
    diel_ref[...] = eye + (4.0 / tb) * final[16:19, 0:3]

    for x in [x0, *x1, xk, xg, *x3, *xa, *x4, xf]:
        x.drain()


def solution(mesh):
    nga, nband = mesh.shape["ga"], mesh.shape["band"]

    def per_device(
        orbitals, energies, projectors, miller_index, recip_scale, species, proj_atom, coupling
    ):
        bands, width = orbitals.shape
        nproj = projectors.shape[0]
        natoms = species.shape[0]
        tb = bands * nband
        rows = 3 * bands
        pchunks = 4
        smw = -(-(3 * tb + 8) // 128) * 128
        axes = ["band"] + ["ga"] * pchunks + ["ga", "ga"]
        axes += ["ga"] * pchunks + ["ga", "band", "band"] + ["ga"] * pchunks + ["ga", "band"]
        sems = []
        for axis in axes:
            sems += [pltpu.SemaphoreType.DMA((mesh.shape[axis],))] * 2
        vmem = pl.BlockSpec(memory_space=pltpu.VMEM)
        return pl.pallas_call(
            functools.partial(kernel, nga, nband, pchunks),
            out_shape=(
                jax.ShapeDtypeStruct((3, bands, width), BF16),
                jax.ShapeDtypeStruct((3, 3), F32),
                jax.ShapeDtypeStruct((9, natoms), F32),
            ),
            in_specs=[pl.BlockSpec(memory_space=pltpu.HBM)] * 8,
            out_specs=(vmem, vmem, vmem),
            scratch_shapes=[
                pltpu.VMEM(orbitals.shape, BF16),
                pltpu.SMEM(energies.shape, F32),
                pltpu.VMEM(miller_index.shape, jnp.int32),
                pltpu.SMEM(recip_scale.shape, F32),
                pltpu.VMEM((1, natoms), jnp.int32),
                pltpu.VMEM((1, nproj), jnp.int32),
                pltpu.SMEM(coupling.shape, F32),
                pltpu.SemaphoreType.DMA((7,)),
                pltpu.VMEM((nproj, width), BF16),
                pltpu.VMEM((nband, bands, width), BF16),
                pltpu.VMEM((tb, width), F32),
                pltpu.VMEM((4 * tb, width), BF16),
                pltpu.VMEM((nga, 4 * bands, nproj), BF16),
                pltpu.VMEM((nga, bands, nproj), BF16),
                pltpu.VMEM((nband, bands, 2 * nproj), BF16),
                pltpu.VMEM((tb, 2 * nproj), F32),
                pltpu.VMEM((nga, bands, 4 * tb), F32),
                pltpu.VMEM((nband, bands, 4 * tb), F32),
                pltpu.VMEM((tb, 4 * tb), F32),
                pltpu.VMEM((nga, rows, nproj), BF16),
                pltpu.VMEM((nga, rows, smw), F32),
                pltpu.VMEM((nga, rows, nproj), BF16),
                pltpu.VMEM((nga, rows, 128), F32),
                pltpu.VMEM((nband, 24, natoms), F32),
                pltpu.VMEM((16, nproj), F32),
                pltpu.SemaphoreType.DMA((pchunks,)),
                *sems,
            ],
            compiler_params=pltpu.CompilerParams(
                collective_id=0, has_side_effects=True, vmem_limit_bytes=67_043_328
            ),
        )(
            orbitals,
            energies,
            projectors,
            miller_index,
            recip_scale,
            species.reshape(1, natoms),
            proj_atom.reshape(1, nproj),
            coupling,
        )

    placed = (
        P(("grp", "band"), "ga"),
        P(("grp", "band")),
        P("grp", "ga"),
        P(None, "ga"),
        P("grp"),
        P(),
        P(),
        P(),
    )
    return jax.shard_map(
        per_device,
        mesh=mesh,
        in_specs=placed,
        out_specs=(P(None, ("grp", "band"), "ga"), P("grp", None), P(None, "grp")),
        check_vma=False,
    )
```

```python
import functools

import jax
import jax.numpy as jnp
from jax import lax
from jax.experimental import pallas as pl
from jax.experimental.pallas import tpu as pltpu
from jax.sharding import PartitionSpec as P

ITERS = 2
BORN_SCALE = 40.0
MESH = pl.DeviceIdType.MESH
F32 = jnp.float32
BF16 = jnp.bfloat16
NT = (((1,), (1,)), ((), ()))
NN = (((1,), (0,)), ((), ()))


def mm(a, b, dims, precision=None):
    return lax.dot_general(a, b, dims, preferred_element_type=F32, precision=precision)


class Exchange:
    def __init__(self, buf, send, recv, axis, n, me, pick=()):
        self.copies = []
        self.arrivals = []
        for off in range(1, n):
            peer = lax.rem(me + off, n)
            src = buf.at[(me,) + pick]
            self.copies.append(
                pltpu.make_async_remote_copy(
                    src_ref=src,
                    dst_ref=src,
                    send_sem=send.at[off],
                    recv_sem=recv.at[me],
                    device_id={axis: peer},
                    device_id_type=MESH,
                )
            )
            other = buf.at[(peer,) + pick]
            self.arrivals.append(
                pltpu.make_async_remote_copy(
                    src_ref=other,
                    dst_ref=other,
                    send_sem=send.at[off],
                    recv_sem=recv.at[peer],
                    device_id={axis: peer},
                    device_id_type=MESH,
                )
            )

    def start(self):
        for copy in self.copies:
            copy.start()
        return self

    def wait(self):
        for arrival in self.arrivals:
            arrival.wait_recv()

    def drain(self):
        for copy in self.copies:
            copy.wait_send()


def total(buf, n):
    acc = buf[0].astype(F32)
    for j in range(1, n):
        acc = acc + buf[j].astype(F32)
    return acc


def kernel(
    nga,
    nband,
    pchunks,
    orb_hbm,
    energy_hbm,
    proj_hbm,
    miller_hbm,
    recip_hbm,
    species_hbm,
    atom_hbm,
    coupling_hbm,
    resp_ref,
    diel_ref,
    born_ref,
    orb_ref,
    energy_ref,
    miller_ref,
    recip_ref,
    species_ref,
    atom_ref,
    coupling_ref,
    lsem,
    pv,
    oall,
    ofull,
    okall,
    r1,
    kk,
    kall,
    kfull,
    gram,
    gall,
    gfull,
    dir3,
    sm3,
    dir4,
    sm4,
    fin,
    pairs,
    psem,
    *sems,
):
    bands, width = orb_ref.shape
    nproj = pv.shape[0]
    tb = bands * nband
    rows = 3 * bands
    ga = lax.axis_index("ga")
    bd = lax.axis_index("band")
    pc = nproj // pchunks

    barrier = pltpu.get_barrier_semaphore()
    for off in range(1, nga):
        pl.semaphore_signal(
            barrier, inc=1, device_id={"ga": lax.rem(ga + off, nga)}, device_id_type=MESH
        )
    for off in range(1, nband):
        pl.semaphore_signal(
            barrier, inc=1, device_id={"band": lax.rem(bd + off, nband)}, device_id_type=MESH
        )
    small = []
    for i, (src, dst) in enumerate(
        [
            (orb_hbm, orb_ref),
            (miller_hbm, miller_ref),
            (recip_hbm, recip_ref),
            (energy_hbm, energy_ref),
            (species_hbm, species_ref),
            (atom_hbm, atom_ref),
            (coupling_hbm, coupling_ref),
        ]
    ):
        small.append(pltpu.make_async_copy(src, dst, lsem.at[i]))
        small[-1].start()
    loads = []
    for k in range(pchunks):
        part = pl.ds(k * pc, pc)
        loads.append(pltpu.make_async_copy(proj_hbm.at[part], pv.at[part], psem.at[k]))
        loads[-1].start()

    it = iter(sems)

    def exchange(buf, axis, pick=()):
        n, me = (nga, ga) if axis == "ga" else (nband, bd)
        return Exchange(buf, next(it), next(it), axis, n, me, pick)

    for load in small:
        load.wait()
    orb = orb_ref[...].astype(F32)
    wave = [miller_ref[d : d + 1, :].astype(F32) * recip_ref[d] for d in range(3)]
    kinetic = 0.5 * (wave[0] * wave[0] + wave[1] * wave[1] + wave[2] * wave[2])
    precond = 1.0 / (1.0 + kinetic)
    stacked = jnp.concatenate(
        [orb] + [wave[d] * orb for d in range(3)] + [precond * orb], axis=0
    ).astype(BF16)

    pl.semaphore_wait(barrier, nga + nband - 2)

    oall[bd] = orb_ref[...]
    x0 = exchange(oall, "band").start()

    x1 = []
    for k in range(pchunks):
        loads[k].wait()
        part = pl.ds(k * pc, pc)
        piece = mm(stacked, pv[part, :], NT)
        r1[ga, :, part] = piece[: 4 * bands].astype(BF16)
        kk[ga, :, part] = piece[4 * bands :].astype(BF16)
        x1.append(exchange(r1, "ga", (slice(None), part)).start())
    xk = exchange(kk, "ga").start()

    band_row = lax.broadcasted_iota(jnp.int32, (bands, 1), 0)
    ecol = jnp.zeros((bands, 1), F32)
    for n in range(bands):
        ecol = jnp.where(band_row == n, energy_ref[n], ecol)
    ecol = jnp.concatenate([ecol] * 3, axis=0)
    shift = kinetic - ecol

    natoms = species_ref.shape[1]
    atoms = lax.broadcasted_iota(jnp.int32, (natoms, nproj), 0)
    onehot = (atoms == atom_ref[...]).astype(BF16)
    species = species_ref[...].astype(F32)
    spec_rows = jnp.concatenate([species] * 8, axis=0).astype(BF16)
    spec = mm(spec_rows, onehot, NN)[0:1]
    nspec, nchan = coupling_ref.shape
    chan = lax.rem(lax.broadcasted_iota(jnp.int32, (1, nproj), 1), nchan)
    strength = jnp.zeros((1, nproj), F32)
    for s in range(nspec):
        for c in range(nchan):
            strength = jnp.where(
                jnp.logical_and(spec == float(s), chan == c), coupling_ref[s, c], strength
            )

    x0.wait()
    for j in range(nband):
        ofull[j * bands : (j + 1) * bands, :] = oall[j].astype(F32)
    every = ofull[...]
    okall[:tb, :] = every.astype(BF16)
    okall[tb : 2 * tb, :] = (precond * every).astype(BF16)
    okall[2 * tb : 3 * tb, :] = (precond * precond * every).astype(BF16)
    okall[3 * tb :, :] = (kinetic * every).astype(BF16)
    gram[ga] = mm(orb_ref[...], okall[...], NT)
    xg = exchange(gram, "ga").start()

    for x in x1:
        x.wait()
    proj = total(r1, nga)
    weighted = (strength * proj).astype(BF16)
    returned = mm(weighted, pv[...], NN)
    inner = orb + returned[:bands]
    comm = jnp.concatenate(
        [wave[d] * inner + returned[(1 + d) * bands : (2 + d) * bands] for d in range(3)], axis=0
    ).astype(BF16)
    comm_float = comm.astype(F32)

    def send_direction(found, buf):
        low = found.astype(BF16)
        out = []
        for k in range(pchunks):
            part = pl.ds(k * pc, pc)
            buf[ga, :, part] = mm(low, pv[part, :], NT).astype(BF16)
            out.append(exchange(buf, "ga", (slice(None), part)).start())
        return out

    scaled = precond * comm_float
    x3 = send_direction(scaled, dir3)
    sm3[ga, :, : 3 * tb] = mm(comm, okall[: 3 * tb, :], NT)
    sm3[ga, :, 3 * tb : 3 * tb + 1] = jnp.sum(scaled * comm_float, axis=1, keepdims=True)
    sm3[ga, :, 3 * tb + 1 : 3 * tb + 2] = jnp.sum(scaled * scaled, axis=1, keepdims=True)
    x3.append(exchange(sm3, "ga").start())

    xk.wait()
    xg.wait()
    kall[bd, :, :nproj] = proj[:bands].astype(BF16)
    kall[bd, :, nproj:] = total(kk, nga).astype(BF16)
    gall[bd] = total(gram, nga)
    xa = [exchange(kall, "band").start(), exchange(gall, "band").start()]
    for x in xa:
        x.wait()
    for j in range(nband):
        kfull[j * bands : (j + 1) * bands, :] = kall[j].astype(F32)
        gfull[j * bands : (j + 1) * bands, :] = gall[j]
    pp = kfull[:, :nproj].astype(BF16)
    kp = kfull[:, nproj:].astype(BF16)
    grams = gfull[...]
    g1, gk, gk2, gkin = [grams[:, q * tb : (q + 1) * tb] for q in range(4)]

    def hi(a, b):
        return mm(a, b, NN, lax.Precision.HIGHEST)

    for x in x3:
        x.wait()
    small3 = total(sm3, nga)
    u, v, w = [small3[:, q * tb : (q + 1) * tb] for q in range(3)]
    ckc = small3[:, 3 * tb : 3 * tb + 1]
    ck2c = small3[:, 3 * tb + 1 : 3 * tb + 2]
    margin_low = u.astype(BF16)
    margin = margin_low.astype(F32)
    a1k, a2k = hi(margin, gk), hi(margin, gk2)
    margin_next = a1k - v
    next_low = margin_next.astype(BF16)
    nxt = next_low.astype(F32)
    b1, bk, bkin = hi(nxt, g1), hi(nxt, gk), hi(nxt, gkin)
    numerator = ckc + jnp.sum(
        margin * (a1k - 2.0 * v - b1) + nxt * u, axis=1, keepdims=True
    )
    diag = (ckc - ck2c - ecol * ck2c) + jnp.sum(
        margin * (a1k - a2k - 2.0 * (v - w) - 2.0 * (b1 - bk))
        + nxt * (2.0 * (u - v) + bkin)
        - ecol * (margin * (a2k - 2.0 * w - 2.0 * bk) + nxt * (2.0 * v + b1)),
        axis=1,
        keepdims=True,
    )
    margin_step = (a1k - a2k) - (v - w) - (b1 - bk) - ecol * (a2k - w - bk)
    dp1 = mm(margin_low, kp, NN) - mm(next_low, pp, NN) - total(dir3, nga)
    dw1 = (strength * dp1).astype(BF16)
    alpha1 = numerator / (
        diag + jnp.sum(dw1.astype(F32) * dp1, axis=1, keepdims=True)
    )
    removed = mm(jnp.concatenate([margin, nxt], axis=0).astype(BF16), okall[:tb, :], NN)
    source = removed[:rows] - comm_float
    search = precond * source - removed[rows:]

    def overlaps(found):
        return [
            jnp.sum(
                found * jnp.concatenate([source[b * bands : (b + 1) * bands]] * 3, axis=0),
                axis=1,
                keepdims=True,
            )
            for b in range(3)
        ]

    def step_of(buf, small, col):
        dp = total(buf, nga)
        dw = (strength * dp).astype(BF16)
        curvature = small[:, col + 1 : col + 2] + jnp.sum(
            dw.astype(F32) * dp, axis=1, keepdims=True
        )
        return dp, dw, small[:, col : col + 1] / curvature

    shifted = shift * search
    image = shifted + mm(dw1, pv[...], NN)
    residual = source - alpha1 * image
    margin3 = margin_next - alpha1 * (margin_step + mm(dw1, kp, NT))
    search2 = (precond * residual).astype(BF16).astype(F32) - mm(
        margin3.astype(BF16), okall[:tb, :], NN
    )
    x4 = send_direction(search2, dir4)
    for b, col in enumerate(overlaps(search)):
        sm4[ga, :, 2 + b : 3 + b] = col
    sm4[ga, :, 0:1] = jnp.sum(residual * search2, axis=1, keepdims=True)
    sm4[ga, :, 1:2] = jnp.sum(shift * search2 * search2, axis=1, keepdims=True)
    for b, col in enumerate(overlaps(search2)):
        sm4[ga, :, 5 + b : 6 + b] = col
    x4.append(exchange(sm4, "ga").start())

    for x in x4:
        x.wait()
    small4 = total(sm4, nga)
    dp2, _, alpha2 = step_of(dir4, small4, 0)
    resp_proj = alpha1 * dp1 + alpha2 * dp2
    pairs[...] = jnp.zeros_like(pairs)
    for a in range(3):
        left = resp_proj[a * bands : (a + 1) * bands]
        for b in range(3):
            right = proj[(1 + b) * bands : (2 + b) * bands]
            pairs[3 * a + b : 3 * a + b + 1, :] = strength * jnp.sum(
                left * right, axis=0, keepdims=True
            )
    born = mm(pairs[...], onehot.astype(F32), NT, lax.Precision.HIGHEST)
    diel = alpha1 * small4[:, 2:5] + alpha2 * small4[:, 5:8]
    fin[bd, 0:16, :] = born
    fin[bd, 16:24, :] = jnp.zeros((8, born.shape[1]), F32)
    for a in range(3):
        fin[bd, 16 + a : 17 + a, 0:3] = jnp.sum(
            diel[a * bands : (a + 1) * bands], axis=0, keepdims=True
        )
    xf = exchange(fin, "band").start()
    response = alpha1 * search + alpha2 * search2
    for a in range(3):
        resp_ref[a] = response[a * bands : (a + 1) * bands].astype(BF16)
    xf.wait()
    final = total(fin, nband)
    born_ref[...] = BORN_SCALE * final[0:9]
    eye = (
        lax.broadcasted_iota(jnp.int32, (3, 3), 0) == lax.broadcasted_iota(jnp.int32, (3, 3), 1)
    ).astype(F32)
    diel_ref[...] = eye + (4.0 / tb) * final[16:19, 0:3]

    for x in [x0, *x1, xk, xg, *x3, *xa, *x4, xf]:
        x.drain()


def finish(resp, diel, born, resp_out, diel_out, born_out, sem):
    copies = [
        pltpu.make_async_copy(resp, resp_out, sem.at[0]),
        pltpu.make_async_copy(diel, diel_out, sem.at[1]),
        pltpu.make_async_copy(born, born_out, sem.at[2]),
    ]
    for copy in copies:
        copy.start()
    for copy in copies:
        copy.wait()


def solution(mesh):
    nga, nband = mesh.shape["ga"], mesh.shape["band"]

    def per_device(
        orbitals, energies, projectors, miller_index, recip_scale, species, proj_atom, coupling
    ):
        bands, width = orbitals.shape
        nproj = projectors.shape[0]
        natoms = species.shape[0]
        tb = bands * nband
        rows = 3 * bands
        pchunks = 2
        smw = -(-(3 * tb + 8) // 128) * 128
        axes = ["band"] + ["ga"] * pchunks + ["ga", "ga"]
        axes += ["ga"] * pchunks + ["ga", "band", "band"] + ["ga"] * pchunks + ["ga", "band"]
        sems = []
        for axis in axes:
            sems += [pltpu.SemaphoreType.DMA((mesh.shape[axis],))] * 2
        vmem = pl.BlockSpec(memory_space=pltpu.VMEM)
        parts = pl.pallas_call(
            functools.partial(kernel, nga, nband, pchunks),
            out_shape=(
                pltpu.VMEM((3, bands, width), BF16),
                pltpu.VMEM((3, 3), F32),
                pltpu.VMEM((9, natoms), F32),
            ),
            in_specs=[pl.BlockSpec(memory_space=pltpu.HBM)] * 8,
            out_specs=(vmem, vmem, vmem),
            scratch_shapes=[
                pltpu.VMEM(orbitals.shape, BF16),
                pltpu.SMEM(energies.shape, F32),
                pltpu.VMEM(miller_index.shape, jnp.int32),
                pltpu.SMEM(recip_scale.shape, F32),
                pltpu.VMEM((1, natoms), jnp.int32),
                pltpu.VMEM((1, nproj), jnp.int32),
                pltpu.SMEM(coupling.shape, F32),
                pltpu.SemaphoreType.DMA((7,)),
                pltpu.VMEM((nproj, width), BF16),
                pltpu.VMEM((nband, bands, width), BF16),
                pltpu.VMEM((tb, width), F32),
                pltpu.VMEM((4 * tb, width), BF16),
                pltpu.VMEM((nga, 4 * bands, nproj), BF16),
                pltpu.VMEM((nga, bands, nproj), BF16),
                pltpu.VMEM((nband, bands, 2 * nproj), BF16),
                pltpu.VMEM((tb, 2 * nproj), F32),
                pltpu.VMEM((nga, bands, 4 * tb), F32),
                pltpu.VMEM((nband, bands, 4 * tb), F32),
                pltpu.VMEM((tb, 4 * tb), F32),
                pltpu.VMEM((nga, rows, nproj), BF16),
                pltpu.VMEM((nga, rows, smw), F32),
                pltpu.VMEM((nga, rows, nproj), BF16),
                pltpu.VMEM((nga, rows, 128), F32),
                pltpu.VMEM((nband, 24, natoms), F32),
                pltpu.VMEM((16, nproj), F32),
                pltpu.SemaphoreType.DMA((pchunks,)),
                *sems,
            ],
            compiler_params=pltpu.CompilerParams(
                collective_id=0, has_side_effects=True, vmem_limit_bytes=67_108_864 - 256 * 1024
            ),
        )(
            orbitals,
            energies,
            projectors,
            miller_index,
            recip_scale,
            species.reshape(1, natoms),
            proj_atom.reshape(1, nproj),
            coupling,
        )
        return pl.pallas_call(
            finish,
            out_shape=tuple(jax.ShapeDtypeStruct(x.shape, x.dtype) for x in parts),
            in_specs=[vmem] * 3,
            out_specs=[pl.BlockSpec(memory_space=pltpu.HBM)] * 3,
            scratch_shapes=[pltpu.SemaphoreType.DMA((3,))],
            compiler_params=pltpu.CompilerParams(vmem_limit_bytes=1024 * 1024),
        )(*parts)

    placed = (
        P(("grp", "band"), "ga"),
        P(("grp", "band")),
        P("grp", "ga"),
        P(None, "ga"),
        P("grp"),
        P(),
        P(),
        P(),
    )
    return jax.shard_map(
        per_device,
        mesh=mesh,
        in_specs=placed,
        out_specs=(P(None, ("grp", "band"), "ga"), P("grp", None), P(None, "grp")),
        check_vma=False,
    )
```
